32 devices in a mesh: dp: 8 (over z, y), tensor: 4 (over x, core).
Axes of the slice: x: 2, y: 2, z: 4, core: 2. Of those that a mesh axis runs over, the one named last changes fastest.
Arguments:
- hidden: bfloat16 [128, 4096], P(('dp', 'tensor')), may hold values from -6 to 6
- shortcut: bfloat16 [128, 4096], P('dp'), may hold values from -6 to 6
- expert_ids: int32 [128, 2], P('dp'), may hold values from 0 to 7, all different within a row; in each aligned block of 16 rows (0 to 15, 16 to 31, ...) at most 6 rows name the same one
- route_weight: float32 [128, 2], P('dp'), may hold values from 0.1 to 1
- dense_gain: float32 [4096], replicated, may hold values from 0.5 to 1.5
- moe_gain: float32 [4096], replicated, may hold values from 0.5 to 1.5
- dense_gate: bfloat16 [4096, 8192], P(None, 'dp'), may hold values from -0.09375 to 0.09375
- dense_lift: bfloat16 [4096, 8192], P(None, 'dp'), may hold values from -0.09375 to 0.09375
- dense_down: bfloat16 [8192, 4096], P('dp'), may hold values from -0.0625 to 0.0625
- expert_gate: bfloat16 [4096, 65536], P(None, ('dp', 'tensor')), may hold values from -0.09375 to 0.09375
- expert_lift: bfloat16 [4096, 65536], P(None, ('dp', 'tensor')), may hold values from -0.09375 to 0.09375
- expert_down: bfloat16 [65536, 4096], P(('dp', 'tensor')), may hold values from -0.0625 to 0.0625
Outputs:
- mixed: bfloat16 [128, 4096], P(('dp', 'tensor'))
The draws below stay inside these ranges and needn't reach their ends.
Inputs may be any that keep to these rules, and one draw needn't show every extreme that they name: `expert_ids`: the 2 experts of a token differ. In each aligned block of 16 rows (the tokens of one index of dp) no expert is named by more than 6 rows, and in every draw some expert is named by exactly 6 rows of some block; every expert is named somewhere.
All inputs are finite; a program needn't handle non-finite values.
Results may differ from the reference program's by a relative error of at most 0.006.
Values may be sent and summed in bfloat16 or wider, within the bound.
A program may use at most 128 MiB of HBM per device.

```python
import math
import jax
import jax.numpy as jnp
import numpy as np
from jax import lax

D = 4096
E = 8
TOP = 2
FF = 8192
FF_E = 8192
TOK_DEV = 16
CAP = 6
SLICE = 2048
TOKENS = 128


def shard_levels(key, extent, split, smallest, largest):
    def one(axis_at, blocks):
        heights = jax.random.uniform(jax.random.fold_in(jax.random.fold_in(key, 6), axis_at), (blocks,), jnp.float32, smallest / len(split), largest / len(split))
        return jnp.repeat(jnp.exp(heights), extent[axis_at] // blocks).reshape((-1,) + (1,) * (len(extent) - axis_at - 1))

    level = one(*split[0])
    for cut in split[1:]:
        level = level * one(*cut)
    return level


def deal_out(key, own, number, rows, amount, top, limit, lean):
    sequence = jax.random.permutation(key, amount)
    packed, usual = portions_of(amount, rows * top, limit, lean, True), portions_of(amount, rows * top, limit, lean, False)
    places = jnp.arange(amount)

    def named(lengths, offset_by):
        used = int((lengths > 0).sum())
        fixed = max(1, used // 4)
        shifted = fixed + (places - fixed + offset_by * (used - fixed)) % max(1, amount - fixed)
        return jnp.zeros((amount,), jnp.int32).at[sequence[jnp.where(places < fixed, places, shifted)]].set(jnp.asarray(lengths, jnp.int32))

    lengths = jnp.where(number % 4 == 0, named(packed, number // 4), named(usual, number - number // 4 - 1))
    mixed = jax.random.permutation(jax.random.fold_in(own, 3), amount)
    giver, sink = mixed[0:amount // 2 * 2:2], mixed[1:amount // 2 * 2:2]
    margin = jnp.minimum(lengths[giver] - 1, limit - lengths[sink]) // 2
    margin = jnp.where((giver == sequence[0]) | (sink == sequence[0]) | (lengths[sink] == 0), 0, jnp.maximum(margin, 0))
    shifted = jax.random.randint(jax.random.fold_in(own, 4), (amount // 2,), 0, 1 << 20) % (margin + 1)
    lengths = lengths.at[giver].add(-shifted).at[sink].add(shifted)
    items = jnp.searchsorted(jnp.cumsum(lengths), jnp.arange(rows * top), side="right").astype(jnp.int32)
    grid = items.reshape(top, rows).T
    grid = grid[jax.random.permutation(jax.random.fold_in(own, 1), rows)]
    offset_by = jax.random.randint(jax.random.fold_in(own, 2), (rows, 1), 0, top)
    return jnp.take_along_axis(grid, (jnp.arange(top)[None, :] + offset_by) % top, axis=1)


def portions_of(number_of, total, most, slope, full):
    weights = [(1 << 20) // math.isqrt(grade ** slope) + 1 for grade in range(1, number_of + 1)]
    largest = most if full else min(most, max(-(-total // number_of), total * weights[0] // sum(weights)))
    least = 1 if total - largest >= number_of - 1 else 0
    counts, surplus = [largest] + [least] * (number_of - 1), total - largest - least * (number_of - 1)
    while surplus > 0:
        movable = [i for i in range(1, number_of) if counts[i] < largest] or [i for i in range(1, number_of) if counts[i] < most]
        pool, remaining = sum([weights[i] for i in movable]), surplus
        for i in movable:
            extra = min(most - counts[i], max(1, remaining * weights[i] // pool), surplus)
            counts[i] = counts[i] + extra
            surplus = surplus - extra
    return np.array(counts)


def scatter_about(own_key, extent, scale, limit, split=(), kind=jnp.bfloat16):
    array = jax.random.normal(own_key, extent, jnp.float32) * scale
    if len(split) > 0:
        array = shard_levels(own_key, extent, split, -0.22, 0.18) * array
    return jnp.clip(array, min=-limit, max=limit).astype(kind)


def setup_inputs(seed: int = 0) -> dict:
    splits = jax.random.split(jax.random.key(seed), 13)
    hidden = scatter_about(splits[0], (TOKENS, D), 1.0, 6.0, ((0, 32),))
    shortcut = scatter_about(splits[1], (TOKENS, D), 1.0, 6.0, ((0, 8),))
    expert_ids_keys = jax.random.split(jax.random.fold_in(splits[2], 1), TOKENS // TOK_DEV)
    expert_ids_turns = jax.random.permutation(jax.random.fold_in(splits[2], 3), TOKENS // TOK_DEV)
    expert_ids = jax.vmap(lambda own, number: deal_out(jax.random.fold_in(splits[2], 2), own, number, TOK_DEV, E, TOP, CAP, 2))(expert_ids_keys, expert_ids_turns).reshape((TOKENS, TOP))
    route_weight = jnp.clip(0.1 + 0.9 * jax.random.uniform(splits[3], (TOKENS, TOP), jnp.float32) ** shard_levels(splits[3], (TOKENS, TOP), ((0, 8),), -0.2, 0.2), 0.1, 1.0)
    dense_gain = jnp.clip(jax.random.uniform(splits[4], (D,), jnp.float32, 0.5, 1.5), 0.5, 1.5)
    moe_gain = jnp.clip(jax.random.uniform(splits[5], (D,), jnp.float32, 0.5, 1.5), 0.5, 1.5)
    dense_gate = scatter_about(splits[6], (D, FF), D ** -0.5, 0.09375, ((1, 8),))
    dense_lift = scatter_about(splits[7], (D, FF), D ** -0.5, 0.09375, ((1, 8),))
    dense_down = scatter_about(splits[8], (FF, D), FF ** -0.5, 0.0625, ((0, 8),))
    expert_gate = scatter_about(splits[9], (D, E * FF_E), D ** -0.5, 0.09375, ((1, 32),))
    expert_lift = scatter_about(splits[10], (D, E * FF_E), D ** -0.5, 0.09375, ((1, 32),))
    expert_down = scatter_about(splits[11], (E * FF_E, D), FF_E ** -0.5, 0.0625, ((0, 32),))
    return {"hidden": hidden, "shortcut": shortcut, "expert_ids": expert_ids, "route_weight": route_weight, "dense_gain": dense_gain, "moe_gain": moe_gain, "dense_gate": dense_gate, "dense_lift": dense_lift, "dense_down": dense_down, "expert_gate": expert_gate, "expert_lift": expert_lift, "expert_down": expert_down}


EPSILON = 1e-05

def normalize(values_in, gain):
    values = values_in.astype(jnp.float32)
    scale = lax.rsqrt(lax.optimization_barrier(jnp.mean(values * values, axis=-1, keepdims=True)) + EPSILON)
    return (values * scale * gain).astype(jnp.bfloat16)

def slot_places(expert_ids):
    blocks = expert_ids.shape[0] // TOK_DEV
    flat = expert_ids.reshape(blocks, TOK_DEV * TOP)
    picked = (flat[:, :, None] == jnp.arange(E, dtype=jnp.int32)[None, None, :]).astype(jnp.int32)
    before = jnp.cumsum(picked, axis=1) - picked
    ranks = lax.optimization_barrier(jnp.sum(before * picked, axis=2))
    return flat * CAP + ranks

def reference(hidden, shortcut, expert_ids, route_weight, dense_gain, moe_gain, dense_gate, dense_lift, dense_down, expert_gate, expert_lift, expert_down):
    normed = normalize(hidden, dense_gain)
    gate_vals = jnp.dot(normed, dense_gate, preferred_element_type=jnp.float32)
    lift_vals = jnp.dot(normed, dense_lift, preferred_element_type=jnp.float32)
    dense_inner = (jax.nn.silu(gate_vals) * lift_vals).astype(jnp.bfloat16)
    dense_out = jnp.dot(dense_inner, dense_down, preferred_element_type=jnp.float32)
    moe_in = normalize(shortcut, moe_gain)
    blocks = TOKENS // TOK_DEV
    places = slot_places(expert_ids)
    chosen = (places[:, :, None] == jnp.arange(E * CAP, dtype=jnp.int32)[None, None, :]).astype(jnp.float32)
    chosen = chosen.reshape(blocks, TOK_DEV, TOP, E * CAP)
    spread = lax.optimization_barrier(jnp.sum(chosen, axis=2))
    weighted = lax.optimization_barrier(jnp.sum(chosen * route_weight.reshape(blocks, TOK_DEV, TOP, 1), axis=2))
    grouped = moe_in.astype(jnp.float32).reshape(blocks, TOK_DEV, D)
    buffer = jnp.einsum('bts,btd->bsd', spread, grouped).astype(jnp.bfloat16).reshape(blocks, E, CAP, D)
    parts = FF_E // SLICE

    def one_expert(expert):
        rows_in = lax.dynamic_index_in_dim(buffer, expert, 1, keepdims=False).reshape(blocks * CAP, D)
        start = expert * FF_E
        gate_part = jnp.dot(rows_in, lax.dynamic_slice_in_dim(expert_gate, start, FF_E, 1), preferred_element_type=jnp.float32)
        lift_part = jnp.dot(rows_in, lax.dynamic_slice_in_dim(expert_lift, start, FF_E, 1), preferred_element_type=jnp.float32)
        inner = (jax.nn.silu(gate_part) * lift_part).astype(jnp.bfloat16)

        def add_part(total, index):
            first = index * SLICE
            term = jnp.dot(lax.dynamic_slice_in_dim(inner, first, SLICE, 1), lax.dynamic_slice_in_dim(expert_down, start + first, SLICE, 0), preferred_element_type=jnp.float32).astype(jnp.bfloat16)
            term = lax.optimization_barrier(term)
            return (total + term.astype(jnp.float32), None)
        return lax.scan(add_part, jnp.zeros((blocks * CAP, D), jnp.float32), jnp.arange(parts, dtype=jnp.int32))[0]
    outputs = lax.map(one_expert, jnp.arange(E, dtype=jnp.int32))
    outputs = outputs.reshape(E, blocks, CAP, D).transpose(1, 0, 2, 3).reshape(blocks, E * CAP, D)
    moe_out = jnp.einsum('bts,bsd->btd', weighted, outputs, precision=lax.Precision.HIGHEST).reshape(TOKENS, D)
    return (hidden.astype(jnp.float32) + dense_out + moe_out).astype(jnp.bfloat16)
```

```python
import functools

import jax
import jax.numpy as jnp
from jax import lax
from jax.experimental import pallas as pl
from jax.experimental.pallas import tpu as pltpu
from jax.sharding import PartitionSpec as P

E = 8
TOP = 2
CAP = 6
CP = 8
EPSILON = 1e-05
MESH = pl.DeviceIdType.MESH
F32 = jnp.float32
BF16 = jnp.bfloat16


def rms_scale(values):
    return lax.rsqrt(jnp.mean(values * values, axis=-1, keepdims=True) + EPSILON)


def gated(rows, gate, lift):
    g = jnp.dot(rows, gate, preferred_element_type=F32)
    v = jnp.dot(rows, lift, preferred_element_type=F32)
    return (g / (1.0 + jnp.exp(-g)) * v).astype(BF16)


def kernel(
    cfg,
    hidden, shortcut, ids, route, dgain, mgain, dg, dl, dd, eg, el, ed,
    out,
    gpool, lpool, dpool, epool,
    ag, stage, xd, inner_d, ds, dland,
    disp, land, xe, inner_e, rs, rsland, ret, retland, fin, finland,
    gsem, lsem, dsem, esem,
    ag_s, ag_r, di_s, di_r, rl_s, rl_r, ds_s, ds_r, rs_s, rs_r, re_s, re_r, fi_s, fi_r,
):
    np_, nt, cw, ns, nd, ne, dc, ec = cfg
    h, D = hidden.shape
    B = shortcut.shape[0]
    Dq = D // nt
    members = np_ // E
    p = lax.axis_index("dp")
    t = lax.axis_index("tensor")
    nb, nc = D // dc, D // ec
    perq = Dq // ec

    def pair(src_g, src_l, i, q):
        slot = lax.rem(q, ns)
        cols = pl.ds(pl.multiple_of(i * cw, cw), cw)
        return (
            pltpu.make_async_copy(src_g.at[:, cols], gpool.at[slot], gsem.at[slot]),
            pltpu.make_async_copy(src_l.at[:, cols], lpool.at[slot], lsem.at[slot]),
        )

    def down_d(c):
        cols = pl.ds(pl.multiple_of(c * dc, dc), dc)
        return pltpu.make_async_copy(dd.at[:, cols], dpool.at[c], dsem.at[c])

    def quarter(c):
        return lax.rem(t + 1 + c // perq, nt)

    def down_e(c):
        start = quarter(c) * Dq + lax.rem(c, perq) * ec
        cols = pl.ds(pl.multiple_of(start, ec), ec)
        return pltpu.make_async_copy(ed.at[:, cols], epool.at[c], esem.at[c])

    def start_pair(src_g, src_l, i, q):
        for copy in pair(src_g, src_l, i, q):
            copy.start()

    barrier = pltpu.get_barrier_semaphore()

    def greet_dp(k, _):
        pl.semaphore_signal(
            barrier, inc=1, device_id=(lax.rem(p + k, np_), t), device_id_type=MESH
        )
        return 0

    lax.fori_loop(1, np_, greet_dp, 0)
    for j in range(1, nt):
        pl.semaphore_signal(
            barrier, inc=1, device_id=(p, lax.rem(t + j, nt)), device_id_type=MESH
        )

    first = min(ns, nd + ne)
    for q in range(min(first, nd)):
        start_pair(dg, dl, q, q)
    for c in range(nb):
        down_d(c).start()
    for q in range(nd, first):
        start_pair(eg, el, q - nd, q)

    hid = hidden[...].astype(F32)
    ag[p] = (hid * rms_scale(hid) * dgain[...]).astype(BF16)
    pl.semaphore_wait(barrier, np_ + nt - 2)

    def ag_copy(k, src):
        return pltpu.make_async_remote_copy(
            src_ref=ag.at[src], dst_ref=ag.at[src], send_sem=ag_s.at[k],
            recv_sem=ag_r.at[src], device_id=(lax.rem(p + k, np_), t), device_id_type=MESH,
        )

    def send_ag(k, _):
        ag_copy(k, p).start()
        return 0

    lax.fori_loop(1, np_, send_ag, 0)

    wide = 128
    col = lax.broadcasted_iota(jnp.int32, (B, wide), 1)
    col_e = lax.shift_right_logical(col, 3)
    col_s = col & 7
    at0 = jnp.where(ids[:, 0:1] == col_e, 1.0, 0.0).astype(F32)
    at1 = jnp.where(ids[:, 1:2] == col_e, 1.0, 0.0).astype(F32)
    named = at0 + at1
    r_i = lax.broadcasted_iota(jnp.int32, (B, B), 0)
    c_i = lax.broadcasted_iota(jnp.int32, (B, B), 1)
    lower = jnp.where(c_i < r_i, 1.0, 0.0).astype(BF16)
    before = jnp.dot(lower, named.astype(BF16), preferred_element_type=F32)
    spread = jnp.where(before.astype(jnp.int32) == col_s, named, 0.0)
    weighted = spread * (at0 * route[:, 0:1] + at1 * route[:, 1:2])

    sc = rms_scale(shortcut[...].astype(F32))
    mine = pl.ds(pl.multiple_of(t * Dq, Dq), Dq)
    moe_q = (shortcut[:, mine].astype(F32) * sc * mgain[:, mine]).astype(BF16)
    spread_t = jnp.transpose(spread)[: E * CP].astype(BF16)
    buf = jnp.dot(spread_t, moe_q, preferred_element_type=F32)
    disp[...] = buf.reshape(E, CP, Dq).astype(BF16)

    def di_copy(k, src):
        to = lax.rem(p + k, np_)
        return pltpu.make_async_remote_copy(
            src_ref=disp.at[to // members], dst_ref=land.at[t, src], send_sem=di_s.at[k],
            recv_sem=di_r.at[src], device_id=(to, t), device_id_type=MESH,
        )

    def send_di(k, _):
        di_copy(k, p).start()
        return 0

    lax.fori_loop(1, np_, send_di, 0)
    land[t, p] = disp[p // members]

    def recv_ag(k, _):
        ag_copy(k, lax.rem(p + k, np_)).wait_recv()
        return 0

    lax.fori_loop(1, np_, recv_ag, 0)
    for s in range(np_):
        stage[s * h : (s + 1) * h, :] = ag[s].astype(F32)
    xd[...] = stage[...].astype(BF16)

    def dense_step(q, _):
        for copy in pair(dg, dl, q, q):
            copy.wait()
        slot = lax.rem(q, ns)
        cols = pl.ds(pl.multiple_of(q * cw, cw), cw)
        inner_d[:, cols] = gated(xd[...], gpool[slot], lpool[slot])
        later = q + ns - nd

        @pl.when(later < ne)
        def _():
            start_pair(eg, el, later, q + ns)

        return 0

    def rl_copy(j, src):
        return pltpu.make_async_remote_copy(
            src_ref=land.at[src], dst_ref=land.at[src], send_sem=rl_s.at[j],
            recv_sem=rl_r.at[src], device_id=(p, lax.rem(t + j, nt)), device_id_type=MESH,
        )

    half = nd // 2
    lax.fori_loop(0, half, dense_step, 0)

    def recv_di(k, _):
        di_copy(k, lax.rem(p + k, np_)).wait_recv()
        return 0

    lax.fori_loop(1, np_, recv_di, 0)
    for j in range(1, nt):
        rl_copy(j, t).start()
    lax.fori_loop(half, nd, dense_step, 0)

    def dense_down_step(c, _):
        down_d(c).wait()
        o = jnp.dot(inner_d[...], dpool[c], preferred_element_type=F32)
        cols = pl.ds(pl.multiple_of(c * dc, dc), dc)
        for s in range(np_):
            ds[s, :, cols] = o[s * h : (s + 1) * h, :].astype(BF16)
        return 0

    lax.fori_loop(0, nb, dense_down_step, 0)

    def ds_copy(k, src):
        to = lax.rem(p + k, np_)
        return pltpu.make_async_remote_copy(
            src_ref=ds.at[to], dst_ref=dland.at[src], send_sem=ds_s.at[k],
            recv_sem=ds_r.at[src], device_id=(to, t), device_id_type=MESH,
        )

    def send_ds(k, _):
        ds_copy(k, p).start()
        return 0

    lax.fori_loop(1, np_, send_ds, 0)

    for j in range(1, nt):
        rl_copy(j, lax.rem(t + j, nt)).wait_recv()
    for q in range(nt):
        xe[:, q * Dq : (q + 1) * Dq] = land[q].astype(F32).reshape(np_ * CP, Dq).astype(BF16)

    def expert_step(i, _):
        q = i + nd
        for copy in pair(eg, el, i, q):
            copy.wait()
        slot = lax.rem(q, ns)
        cols = pl.ds(pl.multiple_of(i * cw, cw), cw)
        inner_e[:, cols] = gated(xe[...], gpool[slot], lpool[slot])

        @pl.when(i + ns < ne)
        def _():
            start_pair(eg, el, i + ns, q + ns)

        return 0

    tail = min(max(ne - ns, 0), ne)
    lax.fori_loop(0, tail, expert_step, 0)
    for c in range(nc):
        down_e(c).start()
    lax.fori_loop(tail, ne, expert_step, 0)

    def rs_copy(j, to, src):
        return pltpu.make_async_remote_copy(
            src_ref=rs.at[to], dst_ref=rsland.at[src], send_sem=rs_s.at[j],
            recv_sem=rs_r.at[src], device_id=(p, lax.rem(t + j, nt)), device_id_type=MESH,
        )

    def expert_down_step(c, _):
        down_e(c).wait()
        o = jnp.dot(inner_e[...], epool[c], preferred_element_type=F32)
        cols = pl.ds(pl.multiple_of(lax.rem(c, perq) * ec, ec), ec)
        rs[quarter(c), :, :, cols] = o.reshape(np_, CP, ec).astype(BF16)
        j = c // perq + 1

        @pl.when((lax.rem(c, perq) == perq - 1) & (j < nt))
        def _():
            rs_copy(j, lax.rem(t + j, nt), t).start()

        return 0

    lax.fori_loop(0, nc, expert_down_step, 0)

    total = rs[t].astype(F32)
    for j in range(1, nt):
        src = lax.rem(t + j, nt)
        rs_copy(j, src, src).wait_recv()
        total = total + rsland[src].astype(F32)
    ret[...] = total.astype(BF16)

    def re_copy(k, src):
        to = lax.rem(p + k, np_)
        return pltpu.make_async_remote_copy(
            src_ref=ret.at[to], dst_ref=retland.at[src], send_sem=re_s.at[k],
            recv_sem=re_r.at[src], device_id=(to, t), device_id_type=MESH,
        )

    def send_re(k, _):
        re_copy(k, p).start()
        return 0

    lax.fori_loop(1, np_, send_re, 0)
    retland[p] = ret[p]

    dland[p] = ds[p]

    def recv_ds(k, _):
        ds_copy(k, lax.rem(p + k, np_)).wait_recv()
        return 0

    lax.fori_loop(1, np_, recv_ds, 0)
    acc = hid
    for s in range(np_):
        acc = acc + dland[s].astype(F32)

    def recv_re(k, _):
        re_copy(k, lax.rem(p + k, np_)).wait_recv()
        return 0

    lax.fori_loop(1, np_, recv_re, 0)
    summed = jnp.sum(retland[...].astype(F32).reshape(E, members, CP, Dq), axis=1)
    moe = jnp.dot(
        weighted[:, : E * CP], summed.reshape(E * CP, Dq),
        precision=lax.Precision.HIGHEST, preferred_element_type=F32,
    )
    for q in range(nt):
        fin[q] = moe[q * h : (q + 1) * h, :]

    def fi_copy(j, src):
        to = lax.rem(t + j, nt)
        return pltpu.make_async_remote_copy(
            src_ref=fin.at[to], dst_ref=finland.at[src], send_sem=fi_s.at[j],
            recv_sem=fi_r.at[src], device_id=(p, to), device_id_type=MESH,
        )

    for j in range(1, nt):
        fi_copy(j, t).start()
    finland[t] = fin[t]
    for j in range(1, nt):
        fi_copy(j, lax.rem(t + j, nt)).wait_recv()
    for q in range(nt):
        cols = slice(q * Dq, (q + 1) * Dq)
        out[:, cols] = (acc[:, cols] + finland[q]).astype(BF16)

    def sent(k, _):
        ag_copy(k, p).wait_send()
        di_copy(k, p).wait_send()
        ds_copy(k, p).wait_send()
        re_copy(k, p).wait_send()
        return 0

    lax.fori_loop(1, np_, sent, 0)
    for j in range(1, nt):
        rl_copy(j, t).wait_send()
        rs_copy(j, lax.rem(t + j, nt), t).wait_send()
        fi_copy(j, t).wait_send()


def local(np_, nt, hidden, shortcut, ids, route, dgain, mgain, dg, dl, dd, eg, el, ed):
    h, D = hidden.shape
    Dq = D // nt
    fd, fe = dg.shape[1], eg.shape[1]
    cw = min(256, fd, fe)
    nd, ne = fd // cw, fe // cw
    ns = min(6, nd + ne)
    dc, ec = min(1024, D), min(512, Dq)
    cfg = (np_, nt, cw, ns, nd, ne, dc, ec)
    dma = pltpu.SemaphoreType.DMA
    vm = pltpu.VMEM
    vspec = pl.BlockSpec(memory_space=pltpu.VMEM)
    aspec = pl.BlockSpec(memory_space=pl.ANY)
    return pl.pallas_call(
        functools.partial(kernel, cfg),
        out_shape=jax.ShapeDtypeStruct((h, D), BF16),
        in_specs=[vspec] * 6 + [aspec] * 6,
        out_specs=vspec,
        scratch_shapes=[
            vm((ns, D, cw), BF16), vm((ns, D, cw), BF16),
            vm((D // dc, fd, dc), BF16), vm((D // ec, fe, ec), BF16),
            vm((np_, h, D), BF16), vm((np_ * h, D), F32), vm((np_ * h, D), BF16),
            vm((np_ * h, fd), BF16), vm((np_, h, D), BF16), vm((np_, h, D), BF16),
            vm((E, CP, Dq), BF16), vm((nt, np_, CP, Dq), BF16), vm((np_ * CP, D), BF16),
            vm((np_ * CP, fe), BF16), vm((nt, np_, CP, Dq), BF16), vm((nt, np_, CP, Dq), BF16),
            vm((np_, CP, Dq), BF16), vm((np_, CP, Dq), BF16),
            vm((nt, h, Dq), F32), vm((nt, h, Dq), F32),
            dma((ns,)), dma((ns,)), dma((D // dc,)), dma((D // ec,)),
            dma((np_,)), dma((np_,)), dma((np_,)), dma((np_,)),
            dma((nt,)), dma((nt,)), dma((np_,)), dma((np_,)),
            dma((nt,)), dma((nt,)), dma((np_,)), dma((np_,)),
            dma((nt,)), dma((nt,)),
        ],
        compiler_params=pltpu.CompilerParams(
            collective_id=0, has_side_effects=True, vmem_limit_bytes=64 * 1024 * 1024 - 65536
        ),
    )(hidden, shortcut, ids, route, dgain.reshape(1, D), mgain.reshape(1, D), dg, dl, dd, eg, el, ed)


def solution(mesh):
    in_specs = (
        P(("dp", "tensor"), None),
        P("dp", None),
        P("dp", None),
        P("dp", None),
        P(),
        P(),
        P(None, "dp"),
        P(None, "dp"),
        P("dp", None),
        P(None, ("dp", "tensor")),
        P(None, ("dp", "tensor")),
        P(("dp", "tensor"), None),
    )
    body = functools.partial(local, mesh.shape["dp"], mesh.shape["tensor"])
    return jax.shard_map(
        body, mesh=mesh, in_specs=in_specs, out_specs=P(("dp", "tensor"), None), check_vma=False
    )
```
